512 devices in a mesh: gx: 32 (over y, x, core), gy: 16 (over z).
Axes of the slice: x: 4, y: 4, z: 16, core: 2. Of those that a mesh axis runs over, the one named last changes fastest.
Arguments:
- snapshots: bfloat16 [131072, 2048], P(('gx', 'gy')), may hold values from -6 to 6
- volume: bfloat16 [65536, 2048], P('gx', 'gy'), may hold values from -6 to 6
- start_basis: bfloat16 [64, 131072], P(None, ('gx', 'gy')), may hold values from -6 to 6
- wake_mask: int32 [2048], P(('gx', 'gy')), may hold values 0 or 1
Outputs:
- plane_modes: float32 [64, 131072], P(None, ('gx', 'gy'))
- wake_modes: float32 [64, 65536], P(None, ('gx', 'gy'))
The draws below stay inside these ranges and needn't reach their ends.
All inputs are finite; a program needn't handle non-finite values. No bound on the sum of `wake_mask` on one device may be relied on, other than what follows from the above.
Results may differ from the reference program's by a relative error of at most 0.018.
Values may be sent and summed in bfloat16 or wider, within the bound.
No kernel may reach another device: no remote copies, remote signals or barrier semaphores. Data moves between devices by JAX's collectives and lax.ppermute only.
A program may use at most 64 MiB of HBM per device.

```python
import jax
import jax.numpy as jnp
from jax import lax

K = 64
S = 2048
ITERS = 3
CBLOCK = 32
PD = 256
POINTS = 131072
CELLS = 65536


def plant(entries, key, low, high):
    longest = entries.shape.index(max(entries.shape))
    spots = []
    for shift in (0, 1):
        where = [jax.random.randint(jax.random.fold_in(key, axis), (), 0, length) for axis, length in enumerate(entries.shape)]
        where[longest] = (where[longest] + shift) % entries.shape[longest]
        spots.append(tuple(where))
    return entries.at[spots[0]].set(low).at[spots[1]].set(high)


def spiked(result, stream_key, source, target, shards_of, factor):
    def block_of(dim):
        return (jnp.arange(result.shape[dim]) // (result.shape[dim] // shards_of)).reshape((-1,) + (1,) * (result.ndim - 1 - dim))

    one_side = jax.random.permutation(stream_key, shards_of)[block_of(target)]
    other_side = (block_of(target) + shards_of // 2) % shards_of
    return jnp.where((block_of(source) == one_side) | (block_of(source) == other_side), factor * result, result)


def block_scale(key, dims, cuts, low, largest):
    loudness = 1.0
    for position, shards_of in cuts:
        heights = jax.random.uniform(jax.random.fold_in(jax.random.fold_in(key, 6), position), (shards_of,), jnp.float32, low / len(cuts), largest / len(cuts))
        loudness = loudness * jnp.repeat(jnp.exp(heights), dims[position] // shards_of).reshape((-1,) + (1,) * (len(dims) - 1 - position))
    return loudness


def bell_draw(own_key, shape, width, most, shards=(), held_as=jnp.bfloat16):
    factor_of = block_scale(own_key, shape, shards, -0.22, 0.18) if shards else 1.0
    entries = jax.random.normal(own_key, shape, jnp.float32) * width * factor_of
    return jnp.minimum(jnp.maximum(entries, -most), most).astype(held_as)


def bell_draw_with(own_key, shape, deviation, limit, cuts, heavy, kind=jnp.bfloat16):
    array = deviation * jax.random.normal(own_key, shape, jnp.float32)
    if cuts:
        array = array * block_scale(own_key, shape, cuts, -0.22, 0.18)
    return jnp.clip(spiked(array, jax.random.fold_in(own_key, 3), *heavy), -limit, limit).astype(kind)


def setup_inputs(seed: int = 0) -> dict:
    key_of = jax.random.split(jax.random.key(seed), 5)
    return {
        "snapshots": bell_draw(key_of[0], (POINTS, S), 1.0, 6.0, ((0, 512),)),
        "volume": bell_draw_with(key_of[1], (CELLS, S), 1.0, 6.0, ((0, 32), (1, 16)), (1, 0, 32, 2.75)),
        "start_basis": bell_draw(key_of[2], (K, POINTS), 1.0, 6.0, ((1, 512),)),
        "wake_mask": plant((jax.random.randint(key_of[3], (CELLS // CBLOCK,), 0, 2) < 1).astype(jnp.int32), jax.random.fold_in(key_of[3], 1), 0, 1),
    }


def gram_and_coeff(basis, snapshots):
    blocks = POINTS // PD
    rows = snapshots.reshape(blocks, PD, S)
    parts = basis.reshape(K, blocks, PD).transpose(1, 0, 2)

    def accumulate(carry, pair):
        block_rows, block_basis = pair
        gram = carry[0] + jnp.dot(block_basis.astype(jnp.float32), block_basis.T.astype(jnp.float32), preferred_element_type=jnp.float32)
        coeff = carry[1] + jnp.dot(block_basis.astype(jnp.float32), block_rows.astype(jnp.float32), preferred_element_type=jnp.float32)
        return ((gram, coeff), None)
    start = (jnp.zeros((K, K), jnp.float32), jnp.zeros((K, S), jnp.float32))
    totals, unused = lax.scan(accumulate, start, (rows, parts))
    return totals

def new_basis(weights_b, snapshots):
    blocks = POINTS // PD
    rows = snapshots.reshape(blocks, PD, S)

    def update(block_rows):
        value = lax.dot_general(weights_b.astype(jnp.float32), block_rows.astype(jnp.float32), (((1,), (1,)), ((), ())), preferred_element_type=jnp.float32)
        return value.astype(jnp.bfloat16)
    pieces = lax.map(update, rows)
    return pieces.transpose(1, 0, 2).reshape(K, POINTS)

def reference(snapshots, volume, start_basis, wake_mask):
    basis = start_basis
    for step in range(ITERS):
        gram, coeff = gram_and_coeff(basis, snapshots)
        lower = jnp.linalg.cholesky(gram)
        weights = jax.scipy.linalg.solve_triangular(lower, coeff, lower=True)
        basis = new_basis(weights.astype(jnp.bfloat16), snapshots)
    gram, coeff = gram_and_coeff(basis, snapshots)
    lower = jnp.linalg.cholesky(gram)
    weights = jax.scipy.linalg.solve_triangular(lower, coeff, lower=True)
    plane_modes = jax.scipy.linalg.solve_triangular(lower, basis.astype(jnp.float32), lower=True) * jnp.sqrt(jnp.float32(POINTS))
    norms = jnp.sqrt(lax.optimization_barrier(jnp.sum(weights * weights, axis=1, keepdims=True)))
    scaled = (weights / norms).astype(jnp.bfloat16)
    projection = lax.dot_general(scaled.astype(jnp.float32), volume.astype(jnp.float32), (((1,), (1,)), ((), ())), preferred_element_type=jnp.float32)
    cell_mask = jnp.repeat(wake_mask, CBLOCK).astype(jnp.float32)
    return (plane_modes, projection * cell_mask[None, :])
```

```python
import functools

import jax
import jax.numpy as jnp
from jax import lax
from jax.experimental import pallas as pl
from jax.experimental.pallas import tpu as pltpu
from jax.sharding import Mesh
from jax.sharding import PartitionSpec as P

ITERS = 3
CBLOCK = 32
PLANE = ("gx_0", "gx_1", "gx_2")
EVERY = ("gx_0", "gx_1", "gx_2", "gy")
PANEL = 4
f32 = jnp.float32
bf16 = jnp.bfloat16
ROW_BY_ROW = (((1,), (1,)), ((), ()))


def whitener(gram):
    n = gram.shape[0]
    blocks = n // 8
    lane = lax.broadcasted_iota(jnp.int32, (8, 2 * n), 1)
    sub = lax.broadcasted_iota(jnp.int32, (8, 2 * n), 0)
    wide = jnp.concatenate([gram, jnp.zeros((n, n), f32)], axis=1)
    rows = [jnp.where(lane == sub + (n + 8 * b), 1.0, wide[8 * b : 8 * b + 8]) for b in range(blocks)]
    scale = [jnp.zeros((8, 2 * n), f32) for _ in range(blocks)]
    for start in range(0, n, PANEL):
        b = start // 8
        cols = [
            [jnp.broadcast_to(rows[r][:, k : k + 1], (8, 2 * n)) for r in range(b, blocks)]
            for k in range(start, start + PANEL)
        ]
        for j in range(PANEL):
            s = (start + j) % 8
            pivot = jnp.broadcast_to(cols[j][0][s : s + 1], (8, 2 * n))
            inverse = 1.0 / pivot
            scale[b] = jnp.where(sub == s, lax.rsqrt(pivot), scale[b])
            line = jnp.broadcast_to(rows[b][s : s + 1], (8, 2 * n)) * inverse
            below = jnp.where(sub > s, cols[j][0], 0.0)
            for i in range(j + 1, PANEL):
                t = (start + i) % 8
                factor = jnp.broadcast_to(cols[j][0][t : t + 1], (8, 2 * n)) * inverse
                cols[i][0] = cols[i][0] - below * factor
                for r in range(1, blocks - b):
                    cols[i][r] = cols[i][r] - cols[j][r] * factor
            rows[b] = rows[b] - below * line
            for r in range(1, blocks - b):
                rows[b + r] = rows[b + r] - cols[j][r] * line
    full = jnp.concatenate([r * s for r, s in zip(rows, scale)], axis=0)
    return full[:, n:]


def high_and_low(value):
    high = value.astype(bf16)
    return high, (value - high.astype(f32)).astype(bf16)


def whiten(gathered, previous, stack, white):
    modes = stack.shape[0] // 3
    half = modes // 2
    for q in range(stack.shape[1] // 128):
        span = slice(128 * q, 128 * q + 128)
        for side in range(2):
            high, low = high_and_low(gathered[2 * q + side, :half, :])
            stack[half * side : half * side + half, span] = high
            stack[modes + half * side : modes + half * side + half, span] = high
            stack[2 * modes + half * side : 2 * modes + half * side + half, span] = low
    if previous is None:
        lines = jnp.concatenate([gathered[p, half : half + 1, :] for p in range(half)], axis=0)
        gram = jnp.concatenate([lines[:, :modes], lines[:, modes:]], axis=0)
    else:
        both = lax.dot_general(stack[modes:, :], previous[...], ROW_BY_ROW, preferred_element_type=f32)
        gram = both[:modes] + both[modes:]
    inverse = whitener(gram)
    high, low = high_and_low(inverse)
    white[...] = jnp.concatenate([high, low, high], axis=1)
    weights = jnp.dot(white[...], stack[...], preferred_element_type=f32)
    return weights, high, low


def project(basis, rows, parts):
    coeff = jnp.dot(basis, rows[...], preferred_element_type=f32).astype(bf16)
    half = coeff.shape[0] // 2
    for q in range(coeff.shape[1] // 128):
        for side in range(2):
            parts[2 * q + side, :half, :] = coeff[half * side : half * side + half, 128 * q : 128 * q + 128]


def first_step(start, rows, parts):
    basis = start[...]
    modes = basis.shape[0]
    half = modes // 2
    gram = lax.dot_general(basis, basis, ROW_BY_ROW, preferred_element_type=f32)
    lines = jnp.concatenate([gram[:half], gram[half:]], axis=1)
    high, low = high_and_low(lines)
    least = (lines - high.astype(f32) - low.astype(f32)).astype(bf16)
    spare = jnp.zeros((parts.shape[1] - half - 3, 128), bf16)
    for p in range(half):
        own = slice(p, p + 1)
        parts[p, half:, :] = jnp.concatenate([high[own], low[own], least[own], spare], axis=0)
    project(basis, rows, parts)


def next_step(with_gram, *refs):
    if with_gram:
        gathered, rows, parts, weights_b, new_basis, stack, white = refs
        previous = None
    else:
        gathered, previous, rows, parts, weights_b, new_basis, stack, white = refs
    weights, _, _ = whiten(gathered, previous, stack, white)
    weights_b[...] = weights.astype(bf16)
    basis = lax.dot_general(weights_b[...], rows[...], ROW_BY_ROW, preferred_element_type=f32).astype(bf16)
    new_basis[...] = basis
    project(basis, rows, parts)


def last_step(root, gathered, previous, basis, cells, mask, plane, wake, stack, white):
    weights, high, low = whiten(gathered, previous, stack, white)
    modes = high.shape[0]
    twice = jnp.concatenate([high, low], axis=0)
    both = jnp.dot(twice, basis[...], preferred_element_type=f32)
    plane[...] = (both[:modes] + both[modes:]) * root
    norms = jnp.sqrt(jnp.sum(weights * weights, axis=1, keepdims=True))
    scaled = (weights / norms).astype(bf16)
    projection = lax.dot_general(scaled, cells[...], ROW_BY_ROW, preferred_element_type=f32)
    wake[...] = projection * mask[...]


def call(body, outs, scratch, *args):
    return pl.pallas_call(
        body,
        out_shape=outs,
        scratch_shapes=scratch,
        name=body.func.__name__ if isinstance(body, functools.partial) else body.__name__,
    )(*args)


def copies_to_each(array, axes):
    copies = jnp.broadcast_to(array, (lax.axis_size(axes), *array.shape))
    return lax.all_to_all(copies, axes, split_axis=0, concat_axis=0, tiled=True)


def summed(parts, with_gram):
    arrived = lax.all_to_all(parts, PLANE, split_axis=0, concat_axis=0, tiled=True)
    own = arrived.astype(f32).sum(axis=0)
    if with_gram:
        half = 32
        gram = own[half : half + 1] + own[half + 1 : half + 2] + own[half + 2 : half + 3]
        own = jnp.concatenate([own[:half], gram, jnp.zeros((7, 128), f32)], axis=0)
    own = copies_to_each(own, "gy").sum(axis=0)
    return copies_to_each(own, PLANE)


def local(snapshots, volume, start_basis, wake_mask):
    points, snaps = snapshots.shape
    modes = start_basis.shape[0]
    half = modes // 2
    pieces = 2 * snaps // 128
    plain = jax.ShapeDtypeStruct((pieces, half, 128), bf16)
    scratch = [pltpu.VMEM((3 * modes, snaps), bf16), pltpu.VMEM((modes, 3 * modes), bf16)]
    parts = call(first_step, jax.ShapeDtypeStruct((pieces, half + 16, 128), bf16), [], start_basis, snapshots)
    gathered = summed(parts, True)
    weights_b = None
    for step in range(ITERS):
        outs = (plain, jax.ShapeDtypeStruct((modes, snaps), bf16), jax.ShapeDtypeStruct((modes, points), bf16))
        given = (gathered,) if weights_b is None else (gathered, weights_b)
        parts, weights_b, basis = call(
            functools.partial(next_step, weights_b is None), outs, scratch, *given, snapshots
        )
        gathered = summed(parts, False)
    own_cells = lax.all_to_all(volume, "gy", split_axis=0, concat_axis=1, tiled=True)
    cell_mask = jnp.repeat(wake_mask, CBLOCK).astype(f32)[None, :]
    total_points = points * lax.axis_size(EVERY)
    outs = (jax.ShapeDtypeStruct((modes, points), f32), jax.ShapeDtypeStruct((modes, own_cells.shape[0]), f32))
    return call(
        functools.partial(last_step, float(total_points) ** 0.5),
        outs, scratch, gathered, weights_b, basis, own_cells, cell_mask,
    )


def solution(mesh):
    finer = Mesh(mesh.devices.reshape(4, 4, 2, mesh.shape["gy"]), EVERY)
    placed = (P(EVERY, None), P(PLANE, "gy"), P(None, EVERY), P(EVERY))
    return jax.shard_map(
        local,
        mesh=finer,
        in_specs=placed,
        out_specs=(P(None, EVERY), P(None, EVERY)),
        check_vma=False,
    )
```
